32 devices in a mesh: row: 4 (over x, core), col: 8 (over z, y).
Axes of the slice: x: 2, y: 2, z: 4, core: 2. Of those that a mesh axis runs over, the one named last changes fastest.
Arguments:
- matrix: float32 [2048, 8192], P('col', 'row'), may hold values from -6 to 6
- basis: float32 [8192, 512], P(('row', 'col')), may hold values from -0.0625 to 0.0625
Outputs:
- root: float32 [512, 512], P('row', 'col')
- right: float32 [2048, 512], P('col')
The draws below stay inside these ranges and needn't reach their ends.
All inputs are finite; a program needn't handle non-finite values.
Results may differ from the reference program's by a relative error of at most 0.00018.
Values sent between devices are 32-bit elements; how exact they have to be, the bound alone decides.
A program may use at most 64 MiB of HBM per device.

```python
import jax
import jax.numpy as jnp
from jax import lax

N = 2048
K = 512
ITERS = 8
M = 8192


def steps_of(own_key, extent, split, smallest, largest):
    def one(axis_at, shards_of):
        draws = jax.random.uniform(jax.random.fold_in(jax.random.fold_in(own_key, 6), axis_at), (shards_of,), jnp.float32, smallest / len(split), largest / len(split))
        return jnp.repeat(jnp.exp(draws), extent[axis_at] // shards_of).reshape((-1,) + (1,) * (len(extent) - axis_at - 1))

    gain = one(*split[0])
    for cut in split[1:]:
        gain = gain * one(*cut)
    return gain


def noise(stream_key, dims, width, bound, cuts=(), kind=jnp.bfloat16):
    level = steps_of(stream_key, dims, cuts, -0.22, 0.18) if cuts else 1.0
    drawn = jax.random.normal(stream_key, dims, jnp.float32) * width * level
    return jnp.minimum(jnp.maximum(drawn, -bound), bound).astype(kind)


def setup_inputs(seed: int = 0) -> dict:
    seeds = jax.random.split(jax.random.key(seed), 3)
    matrix = noise(seeds[0], (N, M), 1.0, 6.0, ((0, 8), (1, 4)), jnp.float32)
    basis = noise(seeds[1], (M, K), M ** -0.5, 0.0625, ((0, 32),), jnp.float32)
    return dict(matrix=matrix, basis=basis)


def reference(matrix, basis):
    highest = lax.Precision.HIGHEST
    proj = lax.dot_general(basis, matrix, (((0,), (1,)), ((), ())), precision=highest)
    gram = jnp.dot(proj, proj.T, precision=highest)
    scale = jnp.sqrt(jnp.sum(gram * gram) + 1e-06)
    ident = jnp.eye(K, dtype=jnp.float32)
    upper = gram / scale
    lower = ident
    for step in range(ITERS):
        middle = 0.5 * (3.0 * ident - jnp.dot(lower, upper, precision=highest))
        upper = jnp.dot(upper, middle, precision=highest)
        lower = jnp.dot(middle, lower, precision=highest)
    root_scale = jnp.sqrt(scale)
    root = upper * root_scale
    right = jnp.dot(proj.T, lower, precision=highest) / root_scale
    return (root, right)
```

```python
import functools

import jax
import jax.numpy as jnp
from jax import lax
from jax.experimental import pallas as pl
from jax.experimental.pallas import tpu as pltpu
from jax.sharding import PartitionSpec as P

ITERS = 8
OUTER = 4
MESH = pl.DeviceIdType.MESH


def split(x):
    hi = x.astype(jnp.bfloat16)
    lo = (x - hi.astype(jnp.float32)).astype(jnp.bfloat16)
    return hi, lo


def dot3(a, b, dims=(((1,), (0,)), ((), ()))):
    dot = functools.partial(lax.dot_general, dimension_numbers=dims, preferred_element_type=jnp.float32)
    return dot(a[0], b[0]) + dot(a[0], b[1]) + dot(a[1], b[0])


def kernel(
    nrow, ncol, matrix, basis, root, right,
    blocks, pieces, total, parts, plane, partial, shares, gram, power,
    basis_send, basis_recv, piece_send, piece_recv, part_send, part_recv,
    proj_send, proj_recv, share_send, share_recv, line_send, line_recv,
    gram_send, gram_recv,
):
    inner = ncol // OUTER
    nplane = nrow * inner
    row, col = lax.axis_index("row"), lax.axis_index("col")
    out, inn = col // inner, lax.rem(col, inner)
    me = row * inner + inn
    cols, depth, width = matrix.shape[0], basis.shape[0], basis.shape[1]
    high = plane.shape[0] // nplane
    tall, wide = width // nplane, width // OUTER

    def plane_peer(k):
        other = lax.rem(me + k, nplane)
        return other, {"row": other // inner, "col": out * inner + lax.rem(other, inner)}

    def line_peer(k):
        other = lax.rem(out + k, OUTER)
        return other, {"row": row, "col": other * inner + inn}

    def remote(src, dst, send, recv, device):
        return pltpu.make_async_remote_copy(
            src_ref=src, dst_ref=dst, send_sem=send, recv_sem=recv, device_id=device, device_id_type=MESH
        )

    barrier = pltpu.get_barrier_semaphore()
    for k in range(1, nplane):
        pl.semaphore_signal(barrier, inc=1, device_id=plane_peer(k)[1], device_id_type=MESH)
    for k in range(1, OUTER):
        pl.semaphore_signal(barrier, inc=1, device_id=line_peer(k)[1], device_id_type=MESH)
    pl.semaphore_wait(barrier, nplane - 1 + OUTER - 1)

    def block_copy(source, step, src):
        way = 0 if step > 0 else 1
        return remote(
            src, blocks.at[source], basis_send.at[source, way], basis_recv.at[source],
            {"row": row, "col": (out + step) * inner + inn},
        )

    def both_ways(step):
        return out < OUTER - 1 if step > 0 else out > 0

    for step in (1, -1):
        @pl.when(both_ways(step))
        def _(step=step):
            block_copy(out, step, basis).start()

    def piece_copy(k, at):
        other = lax.rem(inn + k, inner)
        device = {"row": row, "col": out * inner + other}
        start = pl.multiple_of((at * inner + other) * depth, depth)
        return remote(
            matrix.at[:, pl.ds(start, depth)], pieces.at[k - 1, at],
            piece_send.at[k - 1, at], piece_recv.at[k - 1, at], device,
        )

    for d in range(OUTER):
        for k in range(1, inner):
            piece_copy(k, lax.rem(out + d, OUTER)).start()

    def add_block(at, block, first=False):
        halves = split(block[...])
        for k in range(inner):
            if k == 0:
                start = pl.multiple_of((at * inner + inn) * depth, depth)
                mine = matrix[:, pl.ds(start, depth)]
            else:
                piece_copy(k, at).wait_recv()
                mine = pieces[k - 1, at]
            home = pl.ds(pl.multiple_of(lax.rem(inn + inner - k, inner) * cols, cols), cols)
            got = dot3(split(mine), halves)
            total[home, :] = got if first else total[home, :] + got

    add_block(out, basis, True)
    for d in range(1, OUTER):
        for step in (1, -1):
            source = out - step * d

            @pl.when((source >= 0) & (source < OUTER))
            def _(source=source, step=step):
                block_copy(source, step, blocks.at[source]).wait_recv()

                @pl.when(both_ways(step))
                def _():
                    block_copy(source, step, blocks.at[source]).start()

        for step in (1, -1):
            source = out - step * d

            @pl.when((source >= 0) & (source < OUTER))
            def _(source=source, step=step):
                add_block(source, blocks.at[source])

    copies = []
    for k in range(1, nplane):
        other, device = plane_peer(k)
        copy = remote(
            total.at[pl.ds(pl.multiple_of(other * high, high), high), :], parts.at[k - 1],
            part_send.at[k - 1], part_recv.at[k - 1], device,
        )
        copy.start()
        copies.append(copy)
    own = pl.ds(pl.multiple_of(me * high, high), high)
    mine = total[own, :]
    for k, copy in enumerate(copies):
        copy.wait_recv()
        mine = mine + parts[k]
    plane[own, :] = mine

    def proj_copy(k, at):
        spot = plane.at[pl.ds(pl.multiple_of(at * high, high), high), :]
        return remote(spot, spot, proj_send.at[k - 1], proj_recv.at[k - 1], plane_peer(k)[1])

    for k in range(1, nplane):
        proj_copy(k, me).start()
    for k in range(1, nplane):
        proj_copy(k, lax.rem(me + nplane - k, nplane)).wait_recv()

    proj = split(plane[...])
    partial[...] = dot3(proj, proj, (((0,), (0,)), ((), ())))

    band = pl.ds(pl.multiple_of(me * tall, tall), tall)

    def lanes(at):
        return pl.ds(pl.multiple_of(at * wide, wide), wide)

    shared = []
    for k in range(1, OUTER):
        other, device = line_peer(k)
        copy = remote(
            partial.at[band, lanes(other)], shares.at[k - 1],
            share_send.at[k - 1], share_recv.at[k - 1], device,
        )
        copy.start()
        shared.append(copy)
    mine = partial[band, lanes(out)]
    for k, copy in enumerate(shared):
        copy.wait_recv()
        mine = mine + shares[k]
    gram[band, lanes(out)] = mine

    def line_copy(k, at):
        spot = gram.at[band, lanes(at)]
        return remote(spot, spot, line_send.at[k - 1], line_recv.at[k - 1], line_peer(k)[1])

    for k in range(1, OUTER):
        line_copy(k, out).start()
    for k in range(1, OUTER):
        line_copy(k, lax.rem(out + OUTER - k, OUTER)).wait_recv()

    def gram_copy(k, at):
        spot = gram.at[pl.ds(pl.multiple_of(at * tall, tall), tall), :]
        return remote(spot, spot, gram_send.at[k - 1], gram_recv.at[k - 1], plane_peer(k)[1])

    for k in range(1, nplane):
        gram_copy(k, me).start()
    for k in range(1, nplane):
        gram_copy(k, lax.rem(me + nplane - k, nplane)).wait_recv()

    whole = gram[...]
    scale = jnp.sqrt(jnp.sum(whole * whole, keepdims=True) + 1e-06)
    ident = (
        lax.broadcasted_iota(jnp.int32, (width, width), 0) == lax.broadcasted_iota(jnp.int32, (width, width), 1)
    ).astype(jnp.float32)
    power[...] = whole / scale
    root_scale = jnp.sqrt(scale)
    rows = root.shape[0]
    root[...] = gram[pl.ds(pl.multiple_of(row * rows, rows), rows), :] / scale
    right[...] = plane[pl.ds(pl.multiple_of(inn * cols, cols), cols), :]

    def polar(step, carry):
        now = power[...]
        middle = split(1.5 * ident - 0.5 * now)
        root[...] = dot3(split(root[...]), middle)
        right[...] = dot3(split(right[...]), middle)
        half = dot3(split(now), middle)
        power[...] = dot3(split(half), middle)
        return carry

    lax.fori_loop(0, ITERS - 1, polar, 0)
    middle = split(1.5 * ident - 0.5 * power[...])
    root[...] = dot3(split(root[...]), middle) * root_scale
    right[...] = dot3(split(right[...]), middle) / root_scale

    for step in (1, -1):
        @pl.when(both_ways(step))
        def _(step=step):
            block_copy(out, step, basis).wait_send()
    for d in range(1, OUTER):
        for step in (1, -1):
            source = out - step * d

            @pl.when((source >= 0) & (source < OUTER) & both_ways(step))
            def _(source=source, step=step):
                block_copy(source, step, blocks.at[source]).wait_send()
    for d in range(OUTER):
        for k in range(1, inner):
            piece_copy(k, lax.rem(out + d, OUTER)).wait_send()
    for copy in copies + shared:
        copy.wait_send()
    for k in range(1, nplane):
        proj_copy(k, me).wait_send()
        gram_copy(k, me).wait_send()
    for k in range(1, OUTER):
        line_copy(k, out).wait_send()


def solution(mesh):
    nrow, ncol = mesh.shape["row"], mesh.shape["col"]
    inner = ncol // OUTER
    nplane = nrow * inner

    def local(matrix, basis):
        cols, (depth, width) = matrix.shape[0], basis.shape
        tall = inner * cols
        dma = pltpu.SemaphoreType.DMA
        vmem = pl.BlockSpec(memory_space=pltpu.VMEM)
        root_rows, right = pl.pallas_call(
            functools.partial(kernel, nrow, ncol),
            out_shape=(
                jax.ShapeDtypeStruct((width // nrow, width), jnp.float32),
                jax.ShapeDtypeStruct((cols, width), jnp.float32),
            ),
            in_specs=[vmem, vmem],
            out_specs=(vmem, vmem),
            scratch_shapes=[
                pltpu.VMEM((OUTER, depth, width), jnp.float32),
                pltpu.VMEM((inner - 1, OUTER, cols, depth), jnp.float32),
                pltpu.VMEM((tall, width), jnp.float32),
                pltpu.VMEM((nplane - 1, tall // nplane, width), jnp.float32),
                pltpu.VMEM((tall, width), jnp.float32),
                pltpu.VMEM((width, width), jnp.float32),
                pltpu.VMEM((OUTER - 1, width // nplane, width // OUTER), jnp.float32),
                pltpu.VMEM((width, width), jnp.float32),
                pltpu.VMEM((width, width), jnp.float32),
                dma((OUTER, 2)),
                dma((OUTER,)),
                dma((inner - 1, OUTER)),
                dma((inner - 1, OUTER)),
                dma((nplane - 1,)),
                dma((nplane - 1,)),
                dma((nplane - 1,)),
                dma((nplane - 1,)),
                dma((OUTER - 1,)),
                dma((OUTER - 1,)),
                dma((OUTER - 1,)),
                dma((OUTER - 1,)),
                dma((nplane - 1,)),
                dma((nplane - 1,)),
            ],
            compiler_params=pltpu.CompilerParams(
                collective_id=0, has_side_effects=True, vmem_limit_bytes=56 * 1024 * 1024
            ),
        )(matrix, basis)
        start = lax.axis_index("col") * (width // ncol)
        return lax.dynamic_slice(root_rows, (0, start), (width // nrow, width // ncol)), right

    return jax.shard_map(
        local,
        mesh=mesh,
        in_specs=(P("col", "row"), P(("row", "col"), None)),
        out_specs=(P("row", "col"), P("col", None)),
        check_vma=False,
    )
```

```python
import functools

import jax
import jax.numpy as jnp
from jax import lax
from jax.experimental import pallas as pl
from jax.experimental.pallas import tpu as pltpu
from jax.sharding import PartitionSpec as P

ITERS = 8
OUTER = 4
CHUNKS = 2
MESH = pl.DeviceIdType.MESH


def split(x):
    hi = x.astype(jnp.bfloat16)
    lo = (x - hi.astype(jnp.float32)).astype(jnp.bfloat16)
    return hi, lo


def dot3(a, b, dims=(((1,), (0,)), ((), ()))):
    dot = functools.partial(lax.dot_general, dimension_numbers=dims, preferred_element_type=jnp.float32)
    return dot(a[0], b[0]) + dot(a[0], b[1]) + dot(a[1], b[0])


def kernel(
    nrow, ncol, matrix, basis, root, right, norm,
    blocks, pieces, total, halves, parts, plane, partial, shares, gram, work,
    basis_send, basis_recv, piece_send, piece_recv, half_send, half_recv, part_send, part_recv,
    share_send, share_recv, line_send, line_recv,
    proj_send, proj_recv, mate_send, mate_recv,
    gram_send, gram_recv, twin_send, twin_recv,
):
    inner = ncol // OUTER
    nchip = nrow // 2 * inner
    row, col = lax.axis_index("row"), lax.axis_index("col")
    out, inn = col // inner, lax.rem(col, inner)
    core = lax.rem(row, 2)
    chip = row // 2 * inner + inn
    me = core * nchip + chip
    cols, depth, width = matrix.shape[0], basis.shape[0], basis.shape[1]
    high = plane.shape[0] // (2 * nchip)
    tall, wide = width // (2 * nchip), width // OUTER
    piece = depth // CHUNKS
    mate = {"row": row + 1 - 2 * core, "col": col}

    def chip_at(k):
        return lax.rem(chip + k, nchip)

    def chip_peer(k):
        other = chip_at(k)
        return {"row": other // inner * 2 + core, "col": out * inner + lax.rem(other, inner)}

    def line_peer(k):
        other = lax.rem(out + k, OUTER)
        return other, {"row": row, "col": other * inner + inn}

    def remote(src, dst, send, recv, device):
        return pltpu.make_async_remote_copy(
            src_ref=src, dst_ref=dst, send_sem=send, recv_sem=recv, device_id=device, device_id_type=MESH
        )

    barrier = pltpu.get_barrier_semaphore()
    greeted = [mate] + [chip_peer(k) for k in range(1, nchip)] + [line_peer(k)[1] for k in range(1, OUTER)]
    for device in greeted:
        pl.semaphore_signal(barrier, inc=1, device_id=device, device_id_type=MESH)
    pl.semaphore_wait(barrier, len(greeted))

    def block_copy(source, step, chunk, own=False):
        way = 0 if step > 0 else 1
        lines = pl.ds(chunk * piece, piece)
        here = blocks.at[source, lines, :]
        return remote(
            basis.at[lines, :] if own else here, here,
            basis_send.at[source, way, chunk], basis_recv.at[source, chunk],
            {"row": row, "col": (out + step) * inner + inn},
        )

    def both_ways(step):
        return out < OUTER - 1 if step > 0 else out > 0

    for step in (1, -1):
        @pl.when(both_ways(step))
        def _(step=step):
            for chunk in range(CHUNKS):
                block_copy(out, step, chunk, True).start()

    def piece_copy(k, at):
        other = lax.rem(inn + k, inner)
        device = {"row": row, "col": out * inner + other}
        start = pl.multiple_of((at * inner + other) * depth, depth)
        return remote(
            matrix.at[:, pl.ds(start, depth)], pieces.at[k - 1, at],
            piece_send.at[k - 1, at], piece_recv.at[k - 1, at], device,
        )

    for d in range(OUTER):
        for k in range(1, inner):
            piece_copy(k, lax.rem(out + d, OUTER)).start()

    def add_block(at, block, first=False):
        block_halves = split(block[...])
        for k in range(inner):
            if k == 0:
                start = pl.multiple_of((at * inner + inn) * depth, depth)
                mine = matrix[:, pl.ds(start, depth)]
            else:
                piece_copy(k, at).wait_recv()
                mine = pieces[k - 1, at]
            home = pl.ds(pl.multiple_of(lax.rem(inn + inner - k, inner) * cols, cols), cols)
            got = dot3(split(mine), block_halves)
            total[home, :] = got if first else total[home, :] + got

    add_block(out, basis, True)
    for d in range(1, OUTER):
        for chunk in range(CHUNKS):
            for step in (1, -1):
                source = out - step * d

                @pl.when((source >= 0) & (source < OUTER))
                def _(source=source, step=step, chunk=chunk):
                    block_copy(source, step, chunk).wait_recv()

                    @pl.when(both_ways(step))
                    def _():
                        block_copy(source, step, chunk).start()

        for step in (1, -1):
            source = out - step * d

            @pl.when((source >= 0) & (source < OUTER))
            def _(source=source, step=step):
                add_block(source, blocks.at[source])

    def part(which, at):
        return pl.ds(pl.multiple_of((which * nchip + at) * high, high), high)

    order = list(range(1, nchip)) + [0]

    def half_copy(k):
        return remote(
            total.at[part(1 - core, chip_at(k)), :], halves.at[k], half_send.at[k], half_recv.at[k], mate
        )

    def part_copy(k):
        return remote(
            total.at[part(core, chip_at(k)), :], parts.at[k - 1], part_send.at[k - 1], part_recv.at[k - 1], chip_peer(k)
        )

    for k in order:
        half_copy(k).start()
    for at, k in enumerate(order):
        half_copy(k).wait_recv()
        spot = part(core, chip_at(k))
        total[spot, :] = total[spot, :] + halves[k]
        if at:
            part_copy(order[at - 1]).start()
    mine = total[part(core, chip), :]
    for k in range(1, nchip):
        part_copy(k).wait_recv()
        mine = mine + parts[k - 1]
    plane[part(core, chip), :] = mine

    def gather(buffer, size, send, recv, pair_send, pair_recv):
        def copy(which, at, send_sem, recv_sem, device):
            spot = buffer.at[pl.ds(pl.multiple_of((which * nchip + at) * size, size), size), :]
            return remote(spot, spot, send_sem, recv_sem, device)

        def from_chip(k):
            return lax.rem(chip + nchip - k, nchip)

        def away(k, at):
            return copy(core, at, send.at[k - 1], recv.at[k - 1], chip_peer(k))

        def across(k, which):
            return copy(which, from_chip(k), pair_send.at[k], pair_recv.at[k], mate)

        for k in range(1, nchip):
            away(k, chip).start()
        across(0, core).start()
        for k in range(1, nchip):
            away(k, from_chip(k)).wait_recv()
            across(k, core).start()
        for k in range(nchip):
            across(k, 1 - core).wait_recv()

        def finish():
            for k in range(1, nchip):
                away(k, chip).wait_send()
            for k in range(nchip):
                across(k, core).wait_send()

        return finish

    finish_proj = gather(plane, high, proj_send, proj_recv, mate_send, mate_recv)

    proj = split(plane[...])
    partial[...] = dot3(proj, proj, (((0,), (0,)), ((), ())))

    band = pl.ds(pl.multiple_of(me * tall, tall), tall)

    def lanes(at):
        return pl.ds(pl.multiple_of(at * wide, wide), wide)

    shared = []
    for k in range(1, OUTER):
        other, device = line_peer(k)
        copy = remote(
            partial.at[band, lanes(other)], shares.at[k - 1],
            share_send.at[k - 1], share_recv.at[k - 1], device,
        )
        copy.start()
        shared.append(copy)
    mine = partial[band, lanes(out)]
    for k, copy in enumerate(shared):
        copy.wait_recv()
        mine = mine + shares[k]
    gram[band, lanes(out)] = mine

    def line_copy(k, at):
        spot = gram.at[band, lanes(at)]
        return remote(spot, spot, line_send.at[k - 1], line_recv.at[k - 1], line_peer(k)[1])

    for k in range(1, OUTER):
        line_copy(k, out).start()
    for k in range(1, OUTER):
        line_copy(k, lax.rem(out + OUTER - k, OUTER)).wait_recv()

    finish_gram = gather(gram, tall, gram_send, gram_recv, twin_send, twin_recv)

    whole = gram[...]
    scale = jnp.sqrt(jnp.sum(whole * whole, keepdims=True) + 1e-06)
    ident = (
        lax.broadcasted_iota(jnp.int32, (width, width), 0) == lax.broadcasted_iota(jnp.int32, (width, width), 1)
    ).astype(jnp.float32)
    norm[...] = jnp.broadcast_to(jnp.sqrt(scale), norm.shape)
    rows = root.shape[0]
    work[0:width, :] = whole / scale
    work[width : width + cols, :] = plane[pl.ds(pl.multiple_of(inn * cols, cols), cols), :]
    work[width + cols :, :] = gram[pl.ds(pl.multiple_of(col * rows, rows), rows), :] / scale

    def polar(step, carry):
        middle = split(1.5 * ident - 0.5 * work[0:width, :])
        got = dot3(split(work[...]), middle)
        work[width:, :] = got[width:, :]
        work[0:width, :] = dot3(split(got[:width, :]), middle)
        return carry

    lax.fori_loop(0, ITERS - 1, polar, 0)
    middle = split(1.5 * ident - 0.5 * work[0:width, :])
    got = dot3(split(work[width:, :]), middle)
    right[...] = got[:cols, :]
    root[...] = got[cols:, :]

    for step in (1, -1):
        @pl.when(both_ways(step))
        def _(step=step):
            for chunk in range(CHUNKS):
                block_copy(out, step, chunk, True).wait_send()
    for d in range(1, OUTER):
        for step in (1, -1):
            source = out - step * d

            @pl.when((source >= 0) & (source < OUTER) & both_ways(step))
            def _(source=source, step=step):
                for chunk in range(CHUNKS):
                    block_copy(source, step, chunk).wait_send()
    for d in range(OUTER):
        for k in range(1, inner):
            piece_copy(k, lax.rem(out + d, OUTER)).wait_send()
    for k in range(nchip):
        half_copy(k).wait_send()
    for k in range(1, nchip):
        part_copy(k).wait_send()
    for copy in shared:
        copy.wait_send()
    for k in range(1, OUTER):
        line_copy(k, out).wait_send()
    finish_proj()
    finish_gram()


def solution(mesh):
    nrow, ncol = mesh.shape["row"], mesh.shape["col"]
    inner = ncol // OUTER
    nchip = nrow // 2 * inner

    def local(matrix, basis):
        cols, (depth, width) = matrix.shape[0], basis.shape
        tall = inner * cols
        vmem = pl.BlockSpec(memory_space=pltpu.VMEM)

        def array(*shape):
            return pltpu.VMEM(shape, jnp.float32)

        def pair(*shape):
            return [pltpu.SemaphoreType.DMA(shape)] * 2

        root, right, norm = pl.pallas_call(
            functools.partial(kernel, nrow, ncol),
            out_shape=(
                jax.ShapeDtypeStruct((width // ncol, width), jnp.float32),
                jax.ShapeDtypeStruct((cols, width), jnp.float32),
                jax.ShapeDtypeStruct((8, 128), jnp.float32),
            ),
            in_specs=[vmem, vmem],
            out_specs=(vmem, vmem, vmem),
            scratch_shapes=[
                array(OUTER, depth, width),
                array(inner - 1, OUTER, cols, depth),
                array(tall, width),
                array(nchip, tall // (2 * nchip), width),
                array(nchip - 1, tall // (2 * nchip), width),
                array(tall, width),
                array(width, width),
                array(OUTER - 1, width // (2 * nchip), width // OUTER),
                array(width, width),
                array(width + cols + width // ncol, width),
                pltpu.SemaphoreType.DMA((OUTER, 2, CHUNKS)),
                pltpu.SemaphoreType.DMA((OUTER, CHUNKS)),
                *pair(inner - 1, OUTER),
                *pair(nchip),
                *pair(nchip - 1),
                *pair(OUTER - 1),
                *pair(OUTER - 1),
                *pair(nchip - 1),
                *pair(nchip),
                *pair(nchip - 1),
                *pair(nchip),
            ],
            compiler_params=pltpu.CompilerParams(
                collective_id=0, has_side_effects=True, vmem_limit_bytes=40 * 1024 * 1024
            ),
        )(matrix, basis)
        root_scale = norm[0, 0]
        long = width // nrow
        part = lax.dynamic_slice(root, (0, lax.axis_index("row") * long), (width // ncol, long))
        return part.T * root_scale, right / root_scale

    return jax.shard_map(
        local,
        mesh=mesh,
        in_specs=(P("col", "row"), P(("row", "col"), None)),
        out_specs=(P("row", "col"), P("col", None)),
        check_vma=False,
    )
```

```python
import functools

import jax
import jax.numpy as jnp
from jax import lax
from jax.experimental import pallas as pl
from jax.experimental.pallas import tpu as pltpu
from jax.sharding import PartitionSpec as P

ITERS = 8
OUTER = 4
CHUNKS = 2
LANES = 128
MESH = pl.DeviceIdType.MESH


def split(x):
    hi = x.astype(jnp.bfloat16)
    lo = (x - hi.astype(jnp.float32)).astype(jnp.bfloat16)
    return hi, lo


def dot3(a, b, dims=(((1,), (0,)), ((), ()))):
    dot = functools.partial(lax.dot_general, dimension_numbers=dims, preferred_element_type=jnp.float32)
    return dot(a[0], b[0]) + dot(a[0], b[1]) + dot(a[1], b[0])


def kernel(
    nrow, ncol, matrix, basis, root, right,
    slab, base, blocks, pieces, total, halves, parts, plane, partial, shares, gram, work,
    basis_send, basis_recv, piece_send, piece_recv, half_send, half_recv, part_send, part_recv,
    share_send, share_recv, line_send, line_recv,
    proj_send, proj_recv, mate_send, mate_recv,
    gram_send, gram_recv, twin_send, twin_recv, load,
):
    inner = ncol // OUTER
    nchip = nrow // 2 * inner
    row, col = lax.axis_index("row"), lax.axis_index("col")
    out, inn = col // inner, lax.rem(col, inner)
    core = lax.rem(row, 2)
    chip = row // 2 * inner + inn
    me = core * nchip + chip
    cols, depth, width = matrix.shape[0], basis.shape[0], basis.shape[1]
    high = plane.shape[0] // (2 * nchip)
    tall, wide = width // (2 * nchip), width // OUTER
    piece = depth // CHUNKS
    mate = {"row": row + 1 - 2 * core, "col": col}

    def chip_at(k):
        return lax.rem(chip + k, nchip)

    def chip_peer(k):
        other = chip_at(k)
        return {"row": other // inner * 2 + core, "col": out * inner + lax.rem(other, inner)}

    def line_peer(k):
        other = lax.rem(out + k, OUTER)
        return other, {"row": row, "col": other * inner + inn}

    def remote(src, dst, send, recv, device):
        return pltpu.make_async_remote_copy(
            src_ref=src, dst_ref=dst, send_sem=send, recv_sem=recv, device_id=device, device_id_type=MESH
        )

    loads = [pltpu.make_async_copy(basis, base, load.at[0]), pltpu.make_async_copy(matrix, slab, load.at[1])]
    for copy in loads:
        copy.start()
    barrier = pltpu.get_barrier_semaphore()
    greeted = [mate] + [chip_peer(k) for k in range(1, nchip)] + [line_peer(k)[1] for k in range(1, OUTER)]
    for device in greeted:
        pl.semaphore_signal(barrier, inc=1, device_id=device, device_id_type=MESH)
    pl.semaphore_wait(barrier, len(greeted))

    def block_copy(source, step, chunk, own=False):
        way = 0 if step > 0 else 1
        lines = pl.ds(chunk * piece, piece)
        here = blocks.at[source, lines, :]
        return remote(
            basis.at[lines, :] if own else here, here,
            basis_send.at[source, way, chunk], basis_recv.at[source, chunk],
            {"row": row, "col": (out + step) * inner + inn},
        )

    def both_ways(step):
        return out < OUTER - 1 if step > 0 else out > 0

    for step in (1, -1):
        @pl.when(both_ways(step))
        def _(step=step):
            for chunk in range(CHUNKS):
                block_copy(out, step, chunk, True).start()

    def piece_copy(k, at):
        other = lax.rem(inn + k, inner)
        device = {"row": row, "col": out * inner + other}
        start = pl.multiple_of((at * inner + other) * depth, depth)
        return remote(
            matrix.at[:, pl.ds(start, depth)], pieces.at[k - 1, at],
            piece_send.at[k - 1, at], piece_recv.at[k - 1, at], device,
        )

    for d in range(OUTER):
        for k in range(1, inner):
            piece_copy(k, lax.rem(out + d, OUTER)).start()

    def add_block(at, block, first=False):
        block_halves = split(block[...])
        for k in range(inner):
            if k == 0:
                start = pl.multiple_of((at * inner + inn) * depth, depth)
                mine = slab[:, pl.ds(start, depth)]
            else:
                piece_copy(k, at).wait_recv()
                mine = pieces[k - 1, at]
            home = pl.ds(pl.multiple_of(lax.rem(inn + inner - k, inner) * cols, cols), cols)
            got = dot3(split(mine), block_halves)
            total[home, :] = got if first else total[home, :] + got

    for copy in loads:
        copy.wait()
    add_block(out, base, True)
    for d in range(1, OUTER):
        for chunk in range(CHUNKS):
            for step in (1, -1):
                source = out - step * d

                @pl.when((source >= 0) & (source < OUTER))
                def _(source=source, step=step, chunk=chunk):
                    block_copy(source, step, chunk).wait_recv()

                    @pl.when(both_ways(step))
                    def _():
                        block_copy(source, step, chunk).start()

        for step in (1, -1):
            source = out - step * d

            @pl.when((source >= 0) & (source < OUTER))
            def _(source=source, step=step):
                add_block(source, blocks.at[source])

    def part(which, at):
        return pl.ds(pl.multiple_of((which * nchip + at) * high, high), high)

    order = list(range(1, nchip)) + [0]

    def half_copy(k):
        return remote(
            total.at[part(1 - core, chip_at(k)), :], halves.at[k], half_send.at[k], half_recv.at[k], mate
        )

    def part_copy(k):
        return remote(
            total.at[part(core, chip_at(k)), :], parts.at[k - 1], part_send.at[k - 1], part_recv.at[k - 1], chip_peer(k)
        )

    for k in order:
        half_copy(k).start()
    for at, k in enumerate(order):
        half_copy(k).wait_recv()
        spot = part(core, chip_at(k))
        total[spot, :] = total[spot, :] + halves[k]
        if at:
            part_copy(order[at - 1]).start()
    mine = total[part(core, chip), :]
    for k in range(1, nchip):
        part_copy(k).wait_recv()
        mine = mine + parts[k - 1]
    plane[part(core, chip), :] = mine

    def gather(buffer, size, send, recv, pair_send, pair_recv):
        def copy(which, at, send_sem, recv_sem, device):
            spot = buffer.at[pl.ds(pl.multiple_of((which * nchip + at) * size, size), size), :]
            return remote(spot, spot, send_sem, recv_sem, device)

        def from_chip(k):
            return lax.rem(chip + nchip - k, nchip)

        def away(k, at):
            return copy(core, at, send.at[k - 1], recv.at[k - 1], chip_peer(k))

        def across(k, which):
            return copy(which, from_chip(k), pair_send.at[k], pair_recv.at[k], mate)

        for k in range(1, nchip):
            away(k, chip).start()
        across(0, core).start()
        for k in range(1, nchip):
            away(k, from_chip(k)).wait_recv()
            across(k, core).start()
        for k in range(nchip):
            across(k, 1 - core).wait_recv()

        def finish():
            for k in range(1, nchip):
                away(k, chip).wait_send()
            for k in range(nchip):
                across(k, core).wait_send()

        return finish

    finish_proj = gather(plane, high, proj_send, proj_recv, mate_send, mate_recv)

    proj = split(plane[...])
    around = me * tall // LANES * LANES
    some = split(plane[:, pl.ds(pl.multiple_of(around, LANES), LANES)])
    partial[...] = dot3(some, proj, (((0,), (0,)), ((), ())))

    band = pl.ds(pl.multiple_of(me * tall, tall), tall)
    inside = pl.ds(pl.multiple_of(me * tall - around, tall), tall)

    def lanes(at):
        return pl.ds(pl.multiple_of(at * wide, wide), wide)

    shared = []
    for k in range(1, OUTER):
        other, device = line_peer(k)
        copy = remote(
            partial.at[inside, lanes(other)], shares.at[k - 1],
            share_send.at[k - 1], share_recv.at[k - 1], device,
        )
        copy.start()
        shared.append(copy)
    mine = partial[inside, lanes(out)]
    for k, copy in enumerate(shared):
        copy.wait_recv()
        mine = mine + shares[k]
    gram[band, lanes(out)] = mine

    def line_copy(k, at):
        spot = gram.at[band, lanes(at)]
        return remote(spot, spot, line_send.at[k - 1], line_recv.at[k - 1], line_peer(k)[1])

    for k in range(1, OUTER):
        line_copy(k, out).start()
    for k in range(1, OUTER):
        line_copy(k, lax.rem(out + OUTER - k, OUTER)).wait_recv()

    finish_gram = gather(gram, tall, gram_send, gram_recv, twin_send, twin_recv)

    whole = gram[...]
    scale = jnp.sqrt(jnp.sum(whole * whole, keepdims=True) + 1e-06)
    ident = (
        lax.broadcasted_iota(jnp.int32, (width, width), 0) == lax.broadcasted_iota(jnp.int32, (width, width), 1)
    ).astype(jnp.float32)
    root_scale = jnp.sqrt(scale)
    rows = root.shape[0]
    work[0:width, :] = whole / scale
    work[width : width + cols, :] = plane[pl.ds(pl.multiple_of(inn * cols, cols), cols), :]
    work[width + cols :, :] = gram[pl.ds(pl.multiple_of(col * rows, rows), rows), :] / scale

    def polar(step, carry):
        middle = split(1.5 * ident - 0.5 * work[0:width, :])
        got = dot3(split(work[...]), middle)
        work[width:, :] = got[width:, :]
        work[0:width, :] = dot3(split(got[:width, :]), middle)
        return carry

    lax.fori_loop(0, ITERS - 1, polar, 0)
    middle = split(1.5 * ident - 0.5 * work[0:width, :])
    got = dot3(split(work[width:, :]), middle)
    right[...] = got[:cols, :] / root_scale
    root[...] = got[cols:, :] * root_scale

    for step in (1, -1):
        @pl.when(both_ways(step))
        def _(step=step):
            for chunk in range(CHUNKS):
                block_copy(out, step, chunk, True).wait_send()
    for d in range(1, OUTER):
        for step in (1, -1):
            source = out - step * d

            @pl.when((source >= 0) & (source < OUTER) & both_ways(step))
            def _(source=source, step=step):
                for chunk in range(CHUNKS):
                    block_copy(source, step, chunk).wait_send()
    for d in range(OUTER):
        for k in range(1, inner):
            piece_copy(k, lax.rem(out + d, OUTER)).wait_send()
    for k in range(nchip):
        half_copy(k).wait_send()
    for k in range(1, nchip):
        part_copy(k).wait_send()
    for copy in shared:
        copy.wait_send()
    for k in range(1, OUTER):
        line_copy(k, out).wait_send()
    finish_proj()
    finish_gram()


def solution(mesh):
    nrow, ncol = mesh.shape["row"], mesh.shape["col"]
    inner = ncol // OUTER
    nchip = nrow // 2 * inner

    def local(matrix, basis):
        cols, (depth, width) = matrix.shape[0], basis.shape
        tall = inner * cols
        vmem = pl.BlockSpec(memory_space=pltpu.VMEM)

        def array(*shape):
            return pltpu.VMEM(shape, jnp.float32)

        def pair(*shape):
            return [pltpu.SemaphoreType.DMA(shape)] * 2

        root, right = pl.pallas_call(
            functools.partial(kernel, nrow, ncol),
            out_shape=(
                jax.ShapeDtypeStruct((width // ncol, width), jnp.float32),
                jax.ShapeDtypeStruct((cols, width), jnp.float32),
            ),
            in_specs=[pl.BlockSpec(memory_space=pltpu.HBM)] * 2,
            out_specs=(vmem, vmem),
            scratch_shapes=[
                array(*matrix.shape),
                array(depth, width),
                array(OUTER, depth, width),
                array(inner - 1, OUTER, cols, depth),
                array(tall, width),
                array(nchip, tall // (2 * nchip), width),
                array(nchip - 1, tall // (2 * nchip), width),
                array(tall, width),
                array(LANES, width),
                array(OUTER - 1, width // (2 * nchip), width // OUTER),
                array(width, width),
                array(width + cols + width // ncol, width),
                pltpu.SemaphoreType.DMA((OUTER, 2, CHUNKS)),
                pltpu.SemaphoreType.DMA((OUTER, CHUNKS)),
                *pair(inner - 1, OUTER),
                *pair(nchip),
                *pair(nchip - 1),
                *pair(OUTER - 1),
                *pair(OUTER - 1),
                *pair(nchip - 1),
                *pair(nchip),
                *pair(nchip - 1),
                *pair(nchip),
                pltpu.SemaphoreType.DMA((2,)),
            ],
            compiler_params=pltpu.CompilerParams(
                collective_id=0, has_side_effects=True, vmem_limit_bytes=40 * 1024 * 1024
            ),
        )(matrix, basis)
        long = width // nrow
        part = lax.dynamic_slice(root, (0, lax.axis_index("row") * long), (width // ncol, long))
        return part.T, right

    return jax.shard_map(
        local,
        mesh=mesh,
        in_specs=(P("col", "row"), P(("row", "col"), None)),
        out_specs=(P("row", "col"), P("col", None)),
        check_vma=False,
    )
```
